32 devices in a mesh: groups: 2 (over x), section: 8 (over z, y), head: 2 (over core).
Axes of the slice: x: 2, y: 2, z: 4, core: 2. Of those that a mesh axis runs over, the one named last changes fastest.
Arguments:
- video_tokens: bfloat16 [8192, 1536], P(('groups', 'section', 'head')), parts along dimension 0, may hold values from -6 to 6
- modulation: float32 [6, 1536], P('groups'), parts along dimension 0, may hold values from -3 to 3
- project_weight: bfloat16 [3, 1536, 1536], P(None, None, 'head'), may hold values from -0.15625 to 0.15625
- output_weight: bfloat16 [1536, 1536], P('head'), may hold values from -0.15625 to 0.15625
- norm_gains: float32 [3, 128], replicated, may hold values from 1 to 2
- text_cache: bfloat16 [2, 512, 1536], P(None, 'groups', 'head'), parts along dimension 1, may hold values from -6 to 6
- text_count: int32 [2], P('groups'), parts along dimension 0, may hold values from 1 to 256, as said below
- video_keep: int32 [8192], P('groups'), parts along dimension 0, may hold values 0 or 1
- patch_order: int32 [16], P('groups'), parts along dimension 0, may hold values from 0 to 7, each once
- stale_cache: bfloat16 [2, 8192, 1536], P(None, ('groups', 'section'), 'head'), parts along dimension 1, may hold values from -6 to 6
Outputs:
- updated: bfloat16 [8192, 1536], P(('groups', 'section', 'head')), parts along dimension 0
- fresh_cache: bfloat16 [2, 8192, 1536], P(None, ('groups', 'section'), 'head'), parts along dimension 1
The draws below stay inside these ranges and needn't reach their ends.
There are 2 independent parts, one for each index of `groups`. The reference program is written for one: setup_inputs(seed, part) draws one part's arguments, and reference() takes and returns one part's arrays. A program takes and returns all parts, laid end to end along the dimension named above; an argument that names none is the same for every part. Nothing has to cross between parts.
Inputs may be any that keep to these rules, and one draw needn't show every extreme that they name: The first text_count text tokens are real, the rest are padding. `video_keep`: 1 keeps a video token as a key, 0 marks padding. `patch_order`: each place 0 to 7 is held by exactly one patch.
All inputs are finite; a program needn't handle non-finite values.
Results may differ from the reference program's by a relative error of at most 0.0049.
Values may be sent and summed in bfloat16 or wider, within the bound.
A program may use at most 128 MiB of HBM per device.

```python
import jax
import jax.numpy as jnp
from jax import lax

D = 1536
HEADS = 12
HEAD_DIM = 128
TEXT = 256
PATCH = 512
HID = 1536
SEQ = 4096
N_SECTION = 8


def draw_text_count(key, part):
    short = jax.random.randint(key, (1,), 1, TEXT // 2 + 1, dtype=jnp.int32)
    odd_part = jnp.asarray(part, jnp.int32) % 2 == 1
    return jnp.where(odd_part, jnp.full((1,), TEXT, jnp.int32), short).astype(jnp.int32)


def with_ends(entries, key, low, top_value):
    extent = entries.shape
    place = [jax.random.randint(jax.random.fold_in(key, axis), (), 0, extent[axis]) for axis in range(len(extent))]
    entries = entries.at[tuple(place)].set(low)
    longest = extent.index(max(extent))
    place[longest] = (place[longest] + 1) % extent[longest]
    return entries.at[tuple(place)].set(top_value)


def block_levels(own_key, dims, cuts, least, largest):
    loudness = 1.0
    for position, blocks in cuts:
        steps = jax.random.uniform(jax.random.fold_in(jax.random.fold_in(own_key, 6), position), (blocks,), jnp.float32, least / len(cuts), largest / len(cuts))
        loudness = loudness * jnp.repeat(jnp.exp(steps), dims[position] // blocks).reshape((-1,) + (1,) * (len(dims) - 1 - position))
    return loudness


def normal_values(rng, dims, deviation, most, split=(), kind=jnp.bfloat16):
    result = deviation * jax.random.normal(rng, dims, jnp.float32)
    if split:
        result = result * block_levels(rng, dims, split, -0.22, 0.18)
    return jnp.clip(result, -most, most).astype(kind)


def setup_inputs(seed: int = 0, part: int = 0) -> dict:
    streams_of = jax.random.split(jax.random.key(seed), 11)
    own_keys = jax.random.split(jax.random.fold_in(streams_of[10], part), 11)
    video_tokens = normal_values(own_keys[0], (SEQ, D), 1.0, 6.0, ((0, 16),))
    modulation = normal_values(own_keys[1], (3, D), 0.7, 3.0, (), jnp.float32)
    project_weight = normal_values(streams_of[2], (3, D, HID), D ** -0.5, 0.15625, ((2, 2),))
    output_weight = normal_values(streams_of[3], (HID, D), HID ** -0.5, 0.15625, ((0, 2),))
    norm_gains = jnp.clip(jax.random.uniform(streams_of[4], (3, HEAD_DIM), jnp.float32, 1.0, 2.0), 1.0, 2.0)
    text_cache = normal_values(own_keys[5], (2, TEXT, HID), 1.4, 6.0, ((2, 2),))
    text_count = draw_text_count(jax.random.fold_in(jax.random.fold_in(streams_of[10], part), 71), part)
    video_keep = with_ends((jax.random.randint(own_keys[7], (SEQ,), 0, 4) < 3).astype(jnp.int32), jax.random.fold_in(own_keys[7], 1), 0, 1)
    patch_order = jax.random.permutation(own_keys[8], N_SECTION).astype(jnp.int32)
    stale_cache = normal_values(own_keys[9], (2, SEQ, HID), 1.4, 6.0, ((1, 8), (2, 2)))
    return dict(video_tokens=video_tokens, modulation=modulation, project_weight=project_weight, output_weight=output_weight, norm_gains=norm_gains, text_cache=text_cache, text_count=text_count, video_keep=video_keep, patch_order=patch_order, stale_cache=stale_cache)


epsilon = 1e-06

def widen(array):
    return lax.optimization_barrier(array).astype(jnp.float32)

def layer_norm(values):
    center = lax.optimization_barrier(jnp.mean(values, axis=-1, keepdims=True))
    shifted = values - center
    spread = lax.optimization_barrier(jnp.mean(shifted * shifted, axis=-1, keepdims=True))
    return shifted * lax.rsqrt(spread + epsilon)

def head_norm(inputs, gain_row):
    per_head = inputs.reshape(inputs.shape[0], HEADS, HEAD_DIM)
    scaled = per_head * lax.rsqrt(lax.optimization_barrier(jnp.mean(per_head * per_head, axis=-1, keepdims=True)) + epsilon) * gain_row
    return scaled.astype(jnp.bfloat16)

def reference(video_tokens, modulation, project_weight, output_weight, norm_gains, text_cache, text_count, video_keep, patch_order, stale_cache):
    hidden = video_tokens.astype(jnp.float32)
    normed = (layer_norm(hidden) * (1.0 + modulation[1]) + modulation[0]).astype(jnp.bfloat16)
    projected = jnp.einsum('sd,cdh->csh', widen(normed), project_weight.astype(jnp.float32), precision=lax.Precision.HIGHEST)
    fresh_cache = projected[1:3].astype(jnp.bfloat16)
    queries = head_norm(projected[0], norm_gains[0])
    fresh_keys = head_norm(widen(fresh_cache[0]), norm_gains[1])
    stale_keys = head_norm(stale_cache[0].astype(jnp.float32), norm_gains[1])
    text_keys = head_norm(text_cache[0].astype(jnp.float32), norm_gains[2])
    fresh_values = fresh_cache[1].reshape(SEQ, HEADS, HEAD_DIM)
    stale_values = stale_cache[1].reshape(SEQ, HEADS, HEAD_DIM)
    text_values = text_cache[1].reshape(TEXT, HEADS, HEAD_DIM)
    text_live = jnp.arange(TEXT, dtype=jnp.int32) < text_count[0]
    score_scale = HEAD_DIM ** (-0.5)

    def rows_of(array, patch_index):
        return lax.dynamic_slice_in_dim(array, (patch_index * PATCH).astype(jnp.int32), PATCH, 0)

    def one_patch(patch_index):
        left_place = jnp.maximum(patch_index - 1, 0).astype(jnp.int32)
        right_place = jnp.minimum(patch_index + 1, N_SECTION - 1).astype(jnp.int32)
        own_slot = patch_order[patch_index]
        left_fresh = patch_order[left_place] < own_slot
        right_fresh = patch_order[right_place] < own_slot
        left_keys = jnp.where(left_fresh, rows_of(fresh_keys, left_place), rows_of(stale_keys, left_place))
        right_keys = jnp.where(right_fresh, rows_of(fresh_keys, right_place), rows_of(stale_keys, right_place))
        left_values = jnp.where(left_fresh, rows_of(fresh_values, left_place), rows_of(stale_values, left_place))
        right_values = jnp.where(right_fresh, rows_of(fresh_values, right_place), rows_of(stale_values, right_place))
        key_rows = jnp.concatenate([left_keys, rows_of(fresh_keys, patch_index), right_keys, text_keys], axis=0)
        value_rows = jnp.concatenate([left_values, rows_of(fresh_values, patch_index), right_values, text_values], axis=0)
        key_live = jnp.concatenate([(rows_of(video_keep, left_place) > 0) & (patch_index > 0), rows_of(video_keep, patch_index) > 0, (rows_of(video_keep, right_place) > 0) & (patch_index < N_SECTION - 1), text_live])
        query_rows = rows_of(queries, patch_index)
        scores = jnp.einsum('qhd,khd->hqk', query_rows.astype(jnp.float32), key_rows.astype(jnp.float32), precision=lax.Precision.HIGHEST) * score_scale
        weights = jnp.where(key_live[None, None, :], jnp.exp(scores), 0.0)
        total = lax.optimization_barrier(jnp.sum(weights, axis=-1))
        numerator = jnp.einsum('hqk,khd->qhd', widen(weights.astype(jnp.bfloat16)), value_rows.astype(jnp.float32), precision=lax.Precision.HIGHEST)
        return (numerator / jnp.transpose(total)[:, :, None]).astype(jnp.bfloat16).reshape(PATCH, HID)
    attended = lax.map(one_patch, jnp.arange(N_SECTION, dtype=jnp.int32)).reshape(SEQ, HID)
    mixed = jnp.dot(attended, output_weight, preferred_element_type=jnp.float32)
    updated = (hidden + modulation[2] * mixed).astype(jnp.bfloat16)
    return (updated, fresh_cache)
```

```python
import jax
import jax.numpy as jnp
from jax import lax
from jax.experimental import pallas as pl
from jax.experimental.pallas import tpu as pltpu
from jax.sharding import PartitionSpec as P

epsilon = 1e-06
log2_e = 1.4426950408889634
MESH = pl.DeviceIdType.MESH
f32 = jnp.float32
bf16 = jnp.bfloat16


def dot_nt(a, b):
    return lax.dot_general(a, b, (((1,), (1,)), ((), ())), preferred_element_type=f32)


def head_norm(rows, gain):
    return rows * lax.rsqrt(jnp.mean(rows * rows, axis=-1, keepdims=True) + epsilon) * gain


def kernel(
    order_ref,
    count_ref,
    tokens_ref,
    modulation_ref,
    gains_ref,
    keep_ref,
    weight_hbm,
    output_weight_hbm,
    text_hbm,
    stale_hbm,
    updated_ref,
    fresh_hbm,
    weight,
    output_weight,
    text,
    stale,
    normed,
    raw,
    query,
    query_mate,
    query_far,
    keys,
    values,
    text_keys,
    text_values,
    own_sum,
    mate_sum,
    far_out,
    far_total_out,
    far_in,
    far_total_in,
    back_out,
    back_total_out,
    back_in,
    back_total_in,
    attended,
    mixed_out,
    mixed_in,
    load_sem,
    store_sem,
    normed_sem,
    query_sem,
    forward_sem,
    far_sem,
    far_total_sem,
    back_sem,
    back_total_sem,
    mixed_sem,
):
    count = lax.axis_size("section")
    me = lax.axis_index("section")
    core = lax.axis_index("head")
    other_core = 1 - core
    parity = lax.rem(me, 2)
    mate = me + 1 - 2 * parity
    step = 2 - 4 * parity
    ahead = me + step
    behind = me - step
    has_ahead = jnp.logical_and(ahead >= 0, ahead < count)
    has_behind = jnp.logical_and(behind >= 0, behind < count)
    rows = tokens_ref.shape[0]
    head = gains_ref.shape[1]
    width = weight.shape[2]
    heads = width // head
    units = 2 * heads
    patch = 2 * rows

    loads = [
        pltpu.make_async_copy(weight_hbm.at[c], weight.at[c], load_sem.at[c]) for c in range(3)
    ]
    loads.append(pltpu.make_async_copy(stale_hbm, stale, load_sem.at[3]))
    loads.append(pltpu.make_async_copy(text_hbm, text, load_sem.at[4]))
    loads.append(pltpu.make_async_copy(output_weight_hbm, output_weight, load_sem.at[5]))
    for load in loads:
        load.start()

    barrier = pltpu.get_barrier_semaphore()
    pl.semaphore_signal(barrier, inc=1, device_id={"head": other_core}, device_id_type=MESH)
    pl.semaphore_signal(barrier, inc=1, device_id={"section": mate}, device_id_type=MESH)

    @pl.when(has_ahead)
    def _():
        pl.semaphore_signal(barrier, inc=1, device_id={"section": ahead}, device_id_type=MESH)

    @pl.when(has_behind)
    def _():
        pl.semaphore_signal(barrier, inc=1, device_id={"section": behind}, device_id_type=MESH)

    hidden = tokens_ref[...].astype(f32)
    shifted = hidden - jnp.mean(hidden, axis=-1, keepdims=True)
    spread = jnp.mean(shifted * shifted, axis=-1, keepdims=True)
    normed[0] = (
        shifted * lax.rsqrt(spread + epsilon) * (1.0 + modulation_ref[1:2, :])
        + modulation_ref[0:1, :]
    ).astype(bf16)

    pl.semaphore_wait(
        barrier, 2 + has_ahead.astype(jnp.int32) + has_behind.astype(jnp.int32)
    )

    normed_copy = pltpu.make_async_remote_copy(
        src_ref=normed.at[0],
        dst_ref=normed.at[1],
        send_sem=normed_sem.at[0],
        recv_sem=normed_sem.at[1],
        device_id={"head": other_core},
        device_id_type=MESH,
    )
    normed_copy.start()

    def remote(source, target, sems, unit, device):
        return pltpu.make_async_remote_copy(
            src_ref=source.at[unit],
            dst_ref=target.at[unit],
            send_sem=sems.at[0, unit],
            recv_sem=sems.at[1, unit],
            device_id={"section": device},
            device_id_type=MESH,
        )

    def query_copy(unit):
        return remote(query, query_mate, query_sem, unit, mate)

    def forward_copy(unit, device):
        return remote(query_mate, query_far, forward_sem, unit, device)

    def far_copies(unit, device):
        return (
            remote(far_out, far_in, far_sem, unit, device),
            remote(far_total_out, far_total_in, far_total_sem, unit, device),
        )

    def back_copies(unit):
        return (
            remote(back_out, back_in, back_sem, unit, mate),
            remote(back_total_out, back_total_in, back_total_sem, unit, mate),
        )

    factor = head ** (-0.5) * log2_e
    pair = 2 if heads % 2 == 0 else 1
    span = pair * head

    def columns(step_index):
        return pl.ds(pl.multiple_of(step_index * span, span), span)

    def project_queries(half):
        @pl.loop(0, heads // pair)
        def _(c):
            part = jnp.dot(normed[half], weight[0, :, columns(c)], preferred_element_type=f32)
            for j in range(pair):
                unit = half * heads + c * pair + j
                query[unit] = (
                    head_norm(part[:, j * head : (j + 1) * head], gains_ref[0:1, :]) * factor
                ).astype(bf16)
                query_copy(unit).start()

    def project_caches(half):
        place = core if half == 0 else other_core
        here = pl.ds(pl.multiple_of(place * rows, rows), rows)

        @pl.loop(0, heads // pair)
        def _(c):
            for w in range(2):
                part = jnp.dot(
                    normed[half], weight[1 + w, :, columns(c)], preferred_element_type=f32
                )
                raw[w, here, columns(c)] = part.astype(bf16)

    loads[0].wait()
    project_queries(0)
    loads[1].wait()
    loads[2].wait()
    project_caches(0)
    normed_copy.wait_recv()
    project_queries(1)
    project_caches(1)
    fresh_store = pltpu.make_async_copy(raw, fresh_hbm, store_sem)
    fresh_store.start()
    loads[3].wait()
    loads[4].wait()

    keep_row = keep_ref[pl.ds(me, 1), :].astype(f32)
    keep = jnp.transpose(jnp.broadcast_to(keep_row, (head, patch)))
    text_rows = text.shape[1]
    live = (
        lax.broadcasted_iota(jnp.int32, (text_rows, head), 0) < count_ref[0]
    ).astype(f32)

    @pl.loop(0, heads)
    def _(h):
        lanes = pl.ds(pl.multiple_of(h * head, head), head)
        for version, cache in ((0, raw), (1, stale)):
            keys[version, h] = head_norm(
                cache[0, :, lanes].astype(f32), gains_ref[1:2, :]
            ).astype(bf16)
            values[version, h, :, 0:head] = (cache[1, :, lanes].astype(f32) * keep).astype(bf16)
            values[version, h, :, head : 2 * head] = keep.astype(bf16)
        text_keys[h] = head_norm(text[0, :, lanes].astype(f32), gains_ref[2:3, :]).astype(bf16)
        text_values[h, :, 0:head] = (text[1, :, lanes].astype(f32) * live).astype(bf16)
        text_values[h, :, head : 2 * head] = live.astype(bf16)

    own_slot = order_ref[me]
    mate_version = jnp.where(own_slot < order_ref[mate], 0, 1)
    far_patch = jnp.clip(me - 1 + 2 * parity, 0, count - 1)
    far_version = jnp.where(own_slot < order_ref[far_patch], 0, 1)

    def weighted(queries, key_rows, value_rows):
        weights = jnp.exp2(dot_nt(queries, key_rows)).astype(bf16)
        return jnp.dot(weights, value_rows, preferred_element_type=f32)

    def total_rows(summed):
        return jnp.transpose(summed[:, head : 2 * head])[0:8, :]

    def send_back(unit):
        numerator = mate_sum[unit, :, 0:head]
        totals = total_rows(mate_sum[unit])

        @pl.when(has_ahead)
        def _():
            for copy in far_copies(unit, mate):
                copy.wait_recv()
            back_out[unit] = (numerator + far_in[unit].astype(f32)).astype(bf16)
            back_total_out[unit] = totals + far_total_in[unit]

        @pl.when(jnp.logical_not(has_ahead))
        def _():
            back_out[unit] = numerator.astype(bf16)
            back_total_out[unit] = totals

        for copy in back_copies(unit):
            copy.start()

    @pl.loop(0, units + 3)
    def _(i):
        @pl.when(i < units)
        def _():
            h = lax.rem(i, heads)
            own_sum[i] = weighted(query[i], keys[0, h], values[0, h]) + weighted(
                query[i], text_keys[h], text_values[h]
            )
            query_copy(i).wait_recv()

            @pl.when(has_ahead)
            def _():
                forward_copy(i, ahead).start()

            mate_sum[i] = weighted(query_mate[i], keys[mate_version, h], values[mate_version, h])

        @pl.when(jnp.logical_and(has_behind, jnp.logical_and(i >= 1, i < units + 1)))
        def _():
            unit = i - 1
            h = lax.rem(unit, heads)
            forward_copy(unit, mate).wait_recv()
            summed = weighted(query_far[unit], keys[far_version, h], values[far_version, h])
            far_out[unit] = summed[:, 0:head].astype(bf16)
            far_total_out[unit] = total_rows(summed)
            for copy in far_copies(unit, behind):
                copy.start()

        @pl.when(i >= heads + 3)
        def _():
            send_back(i - 3)

    @pl.loop(0, heads)
    def _(i):
        send_back(i)

    def gather_back(half):
        @pl.loop(0, heads)
        def _(h):
            unit = half * heads + h
            for copy in back_copies(unit):
                copy.wait_recv()
            total = jnp.transpose(
                jnp.broadcast_to(back_total_in[unit, 0:1, :], (head, rows))
            )
            mine = own_sum[unit]
            attended[half, :, pl.ds(pl.multiple_of(h * head, head), head)] = (
                (mine[:, 0:head] + back_in[unit].astype(f32))
                / (mine[:, head : 2 * head] + total)
            ).astype(bf16)

    mixed_copy = pltpu.make_async_remote_copy(
        src_ref=mixed_out,
        dst_ref=mixed_in,
        send_sem=mixed_sem.at[0],
        recv_sem=mixed_sem.at[1],
        device_id={"head": other_core},
        device_id_type=MESH,
    )
    full = output_weight.shape[1]
    wide = 512 if full % 512 == 0 else full

    gather_back(1)
    loads[5].wait()

    @pl.loop(0, full // wide)
    def _(c):
        here = pl.ds(pl.multiple_of(c * wide, wide), wide)
        mixed_out[:, here] = jnp.dot(
            attended[1], output_weight[:, here], preferred_element_type=f32
        ).astype(bf16)

    mixed_copy.start()
    gather_back(0)
    mixed_copy.wait_recv()

    @pl.loop(0, full // wide)
    def _(c):
        here = pl.ds(pl.multiple_of(c * wide, wide), wide)
        mixed = jnp.dot(attended[0], output_weight[:, here], preferred_element_type=f32)
        mixed = mixed + mixed_in[:, here].astype(f32)
        updated_ref[:, here] = (
            tokens_ref[:, here].astype(f32) + modulation_ref[2:3, here] * mixed
        ).astype(bf16)

    fresh_store.wait()
    normed_copy.wait_send()
    mixed_copy.wait_send()

    @pl.loop(0, units)
    def _(i):
        query_copy(i).wait_send()
        for copy in back_copies(i):
            copy.wait_send()

        @pl.when(has_ahead)
        def _():
            forward_copy(i, mate).wait_send()

        @pl.when(has_behind)
        def _():
            for copy in far_copies(i, mate):
                copy.wait_send()


def on_device(
    video_tokens,
    modulation,
    project_weight,
    output_weight,
    norm_gains,
    text_cache,
    text_count,
    video_keep,
    patch_order,
    stale_cache,
):
    head = norm_gains.shape[1]
    rows, model = video_tokens.shape
    width = project_weight.shape[2]
    patch = stale_cache.shape[1]
    text_rows = text_cache.shape[1]
    heads = width // head
    units = 2 * heads
    smem = pl.BlockSpec(memory_space=pltpu.SMEM)
    vmem = pl.BlockSpec(memory_space=pltpu.VMEM)
    hbm = pl.BlockSpec(memory_space=pl.ANY)
    unit_rows = pltpu.VMEM((units, rows, head), bf16)
    unit_totals = pltpu.VMEM((units, 8, rows), f32)
    unit_sums = pltpu.VMEM((units, rows, 2 * head), f32)
    unit_sems = pltpu.SemaphoreType.DMA((2, units))
    return pl.pallas_call(
        kernel,
        out_shape=(
            jax.ShapeDtypeStruct(video_tokens.shape, bf16),
            jax.ShapeDtypeStruct(stale_cache.shape, bf16),
        ),
        in_specs=[smem, smem, vmem, vmem, vmem, vmem, hbm, hbm, hbm, hbm],
        out_specs=(vmem, hbm),
        scratch_shapes=[
            pltpu.VMEM(project_weight.shape, bf16),
            pltpu.VMEM(output_weight.shape, bf16),
            pltpu.VMEM(text_cache.shape, bf16),
            pltpu.VMEM(stale_cache.shape, bf16),
            pltpu.VMEM((2, rows, model), bf16),
            pltpu.VMEM(stale_cache.shape, bf16),
            unit_rows,
            unit_rows,
            unit_rows,
            pltpu.VMEM((2, heads, patch, head), bf16),
            pltpu.VMEM((2, heads, patch, 2 * head), bf16),
            pltpu.VMEM((heads, text_rows, head), bf16),
            pltpu.VMEM((heads, text_rows, 2 * head), bf16),
            unit_sums,
            unit_sums,
            unit_rows,
            unit_totals,
            unit_rows,
            unit_totals,
            unit_rows,
            unit_totals,
            unit_rows,
            unit_totals,
            pltpu.VMEM((2, rows, width), bf16),
            pltpu.VMEM((rows, model), bf16),
            pltpu.VMEM((rows, model), bf16),
            pltpu.SemaphoreType.DMA((6,)),
            pltpu.SemaphoreType.DMA,
            pltpu.SemaphoreType.DMA((2,)),
            unit_sems,
            unit_sems,
            unit_sems,
            unit_sems,
            unit_sems,
            unit_sems,
            pltpu.SemaphoreType.DMA((2,)),
        ],
        compiler_params=pltpu.CompilerParams(
            collective_id=0, has_side_effects=True, vmem_limit_bytes=60 * 1024 * 1024
        ),
    )(
        patch_order,
        text_count,
        video_tokens,
        modulation,
        norm_gains,
        video_keep.reshape(-1, patch),
        project_weight,
        output_weight,
        text_cache,
        stale_cache,
    )


def solution(mesh):
    placed = (
        P(("groups", "section", "head"), None),
        P("groups", None),
        P(None, None, "head"),
        P("head", None),
        P(),
        P(None, "groups", "head"),
        P("groups"),
        P("groups"),
        P("groups"),
        P(None, ("groups", "section"), "head"),
    )
    return jax.shard_map(
        on_device,
        mesh=mesh,
        in_specs=placed,
        out_specs=(P(("groups", "section", "head"), None), P(None, ("groups", "section"), "head")),
        check_vma=False,
    )
```

```python
import jax
import jax.numpy as jnp
from jax import lax
from jax.experimental import pallas as pl
from jax.experimental.pallas import tpu as pltpu
from jax.sharding import PartitionSpec as P

epsilon = 1e-06
log2_e = 1.4426950408889634
MESH = pl.DeviceIdType.MESH
f32 = jnp.float32
bf16 = jnp.bfloat16


def dot_nt(a, b):
    return lax.dot_general(a, b, (((1,), (1,)), ((), ())), preferred_element_type=f32)


def head_norm(rows, gain):
    return rows * lax.rsqrt(jnp.mean(rows * rows, axis=-1, keepdims=True) + epsilon) * gain


def kernel(
    order_ref,
    count_ref,
    tokens_hbm,
    modulation_hbm,
    gains_hbm,
    keep_hbm,
    weight_hbm,
    output_weight_hbm,
    text_hbm,
    stale_hbm,
    updated_ref,
    raw,
    tokens_ref,
    modulation_ref,
    gains_ref,
    keep_ref,
    weight,
    output_weight,
    text,
    stale,
    normed,
    query,
    query_mate,
    query_far,
    keys,
    values,
    text_keys,
    text_values,
    own_sum,
    mate_sum,
    far_out,
    far_total_out,
    far_in,
    far_total_in,
    back_out,
    back_total_out,
    back_in,
    back_total_in,
    attended,
    mixed_out,
    mixed_in,
    load_sem,
    normed_sem,
    query_sem,
    forward_sem,
    far_sem,
    far_total_sem,
    back_sem,
    back_total_sem,
    mixed_sem,
):
    count = lax.axis_size("section")
    me = lax.axis_index("section")
    core = lax.axis_index("head")
    other_core = 1 - core
    parity = lax.rem(me, 2)
    mate = me + 1 - 2 * parity
    step = 2 - 4 * parity
    ahead = me + step
    behind = me - step
    has_ahead = jnp.logical_and(ahead >= 0, ahead < count)
    has_behind = jnp.logical_and(behind >= 0, behind < count)
    rows = tokens_hbm.shape[0]
    head = gains_ref.shape[1]
    width = weight.shape[2]
    heads = width // head
    units = 2 * heads
    patch = 2 * rows

    loads = [
        pltpu.make_async_copy(weight_hbm.at[c], weight.at[c], load_sem.at[c]) for c in range(3)
    ]
    loads.append(pltpu.make_async_copy(stale_hbm, stale, load_sem.at[3]))
    loads.append(pltpu.make_async_copy(text_hbm, text, load_sem.at[4]))
    loads.append(pltpu.make_async_copy(output_weight_hbm, output_weight, load_sem.at[5]))
    small = [
        pltpu.make_async_copy(source, target, load_sem.at[6 + place])
        for place, (source, target) in enumerate(
            (
                (tokens_hbm, tokens_ref),
                (modulation_hbm, modulation_ref),
                (gains_hbm, gains_ref),
                (keep_hbm, keep_ref),
            )
        )
    ]
    for load in small:
        load.start()
    loads[0].start()

    barrier = pltpu.get_barrier_semaphore()
    pl.semaphore_signal(barrier, inc=1, device_id={"head": other_core}, device_id_type=MESH)
    pl.semaphore_signal(barrier, inc=1, device_id={"section": mate}, device_id_type=MESH)

    @pl.when(has_ahead)
    def _():
        pl.semaphore_signal(barrier, inc=1, device_id={"section": ahead}, device_id_type=MESH)

    @pl.when(has_behind)
    def _():
        pl.semaphore_signal(barrier, inc=1, device_id={"section": behind}, device_id_type=MESH)

    for load in small:
        load.wait()
    hidden = tokens_ref[...].astype(f32)
    shifted = hidden - jnp.mean(hidden, axis=-1, keepdims=True)
    spread = jnp.mean(shifted * shifted, axis=-1, keepdims=True)
    normed[0] = (
        shifted * lax.rsqrt(spread + epsilon) * (1.0 + modulation_ref[1:2, :])
        + modulation_ref[0:1, :]
    ).astype(bf16)

    pl.semaphore_wait(
        barrier, 2 + has_ahead.astype(jnp.int32) + has_behind.astype(jnp.int32)
    )

    normed_copy = pltpu.make_async_remote_copy(
        src_ref=normed.at[0],
        dst_ref=normed.at[1],
        send_sem=normed_sem.at[0],
        recv_sem=normed_sem.at[1],
        device_id={"head": other_core},
        device_id_type=MESH,
    )
    normed_copy.start()

    def remote(source, target, sems, unit, device):
        return pltpu.make_async_remote_copy(
            src_ref=source.at[unit],
            dst_ref=target.at[unit],
            send_sem=sems.at[0, unit],
            recv_sem=sems.at[1, unit],
            device_id={"section": device},
            device_id_type=MESH,
        )

    def query_copy(unit):
        return remote(query, query_mate, query_sem, unit, mate)

    def forward_copy(unit, device):
        return remote(query_mate, query_far, forward_sem, unit, device)

    def far_copies(unit, device):
        return (
            remote(far_out, far_in, far_sem, unit, device),
            remote(far_total_out, far_total_in, far_total_sem, unit, device),
        )

    def back_copies(unit):
        return (
            remote(back_out, back_in, back_sem, unit, mate),
            remote(back_total_out, back_total_in, back_total_sem, unit, mate),
        )

    factor = head ** (-0.5) * log2_e
    pair = 2 if heads % 2 == 0 else 1
    span = pair * head

    def columns(step_index):
        return pl.ds(pl.multiple_of(step_index * span, span), span)

    def project_queries(half):
        @pl.loop(0, heads // pair)
        def _(c):
            part = jnp.dot(normed[half], weight[0, :, columns(c)], preferred_element_type=f32)
            for j in range(pair):
                unit = half * heads + c * pair + j
                query[unit] = (
                    head_norm(part[:, j * head : (j + 1) * head], gains_ref[0:1, :]) * factor
                ).astype(bf16)
                query_copy(unit).start()

    early = min(3, heads)

    def forward(unit):
        query_copy(unit).wait_recv()

        @pl.when(has_ahead)
        def _():
            forward_copy(unit, ahead).start()

    for load in loads[1:]:
        load.start()
    loads[0].wait()
    project_queries(0)
    normed_copy.wait_recv()
    project_queries(1)
    loads[1].wait()
    loads[2].wait()
    own_rows = pl.ds(pl.multiple_of(core * rows, rows), rows)
    other_rows = pl.ds(pl.multiple_of(other_core * rows, rows), rows)

    @pl.loop(0, heads // pair)
    def _(c):
        for w in range(2):
            part = jnp.dot(
                normed[...].reshape(patch, normed.shape[2]),
                weight[1 + w, :, columns(c)],
                preferred_element_type=f32,
            ).astype(bf16)
            raw[w, own_rows, columns(c)] = part[0:rows]
            raw[w, other_rows, columns(c)] = part[rows:patch]

        @pl.when(c < early)
        def _():
            forward(c)

    @pl.loop(min(early, heads // pair), early)
    def _(i):
        forward(i)

    loads[3].wait()
    loads[4].wait()

    keep_row = keep_ref[pl.ds(pl.multiple_of(me * patch, patch), patch)].astype(f32)
    keep = jnp.transpose(jnp.broadcast_to(keep_row[None, :], (head, patch)))
    text_rows = text.shape[1]
    live = (
        lax.broadcasted_iota(jnp.int32, (text_rows, head), 0) < count_ref[0]
    ).astype(f32)

    @pl.loop(0, heads)
    def _(h):
        lanes = pl.ds(pl.multiple_of(h * head, head), head)
        for version, cache in ((0, raw), (1, stale)):
            keys[version, h] = head_norm(
                cache[0, :, lanes].astype(f32), gains_ref[1:2, :]
            ).astype(bf16)
            values[version, h, :, 0:head] = (cache[1, :, lanes].astype(f32) * keep).astype(bf16)
            values[version, h, :, head : 2 * head] = keep.astype(bf16)
        text_keys[h] = head_norm(text[0, :, lanes].astype(f32), gains_ref[2:3, :]).astype(bf16)
        text_values[h, :, 0:head] = (text[1, :, lanes].astype(f32) * live).astype(bf16)
        text_values[h, :, head : 2 * head] = live.astype(bf16)

    own_slot = order_ref[me]
    mate_version = jnp.where(own_slot < order_ref[mate], 0, 1)
    far_patch = jnp.clip(me - 1 + 2 * parity, 0, count - 1)
    far_version = jnp.where(own_slot < order_ref[far_patch], 0, 1)

    def weighted(queries, key_rows, value_rows):
        weights = jnp.exp2(dot_nt(queries, key_rows)).astype(bf16)
        return jnp.dot(weights, value_rows, preferred_element_type=f32)

    def total_rows(summed):
        return jnp.transpose(summed[:, head : 2 * head])[0:1, :]

    def send_back(unit):
        numerator = mate_sum[unit, :, 0:head]
        totals = total_rows(mate_sum[unit])

        @pl.when(has_ahead)
        def _():
            for copy in far_copies(unit, mate):
                copy.wait_recv()
            back_out[unit] = (numerator + far_in[unit].astype(f32)).astype(bf16)
            back_total_out[unit] = totals + far_total_in[unit]

        @pl.when(jnp.logical_not(has_ahead))
        def _():
            back_out[unit] = numerator.astype(bf16)
            back_total_out[unit] = totals

        for copy in back_copies(unit):
            copy.start()

    ahead_backs = min(2, heads)

    @pl.loop(early, units + 2 * early)
    def _(i):
        @pl.when(i < units)
        def _():
            forward(i)

        unit = i - early

        @pl.when(unit < units)
        def _():
            h = lax.rem(unit, heads)

            @pl.when(has_behind)
            def _():
                forward_copy(unit, mate).wait_recv()
                summed = weighted(query_far[unit], keys[far_version, h], values[far_version, h])
                far_out[unit] = summed[:, 0:head].astype(bf16)
                far_total_out[unit] = total_rows(summed)
                for copy in far_copies(unit, behind):
                    copy.start()

            mate_sum[unit] = weighted(
                query_mate[unit], keys[mate_version, h], values[mate_version, h]
            )
            own_sum[unit] = weighted(query[unit], keys[0, h], values[0, h]) + weighted(
                query[unit], text_keys[h], text_values[h]
            )

        @pl.when(jnp.logical_and(i >= units - ahead_backs, i < units))
        def _():
            send_back(i - units + ahead_backs)

        @pl.when(i >= heads + 2 * early)
        def _():
            send_back(i - 2 * early)

    @pl.loop(ahead_backs, heads)
    def _(i):
        send_back(i)

    def gather_back(half):
        @pl.loop(0, heads)
        def _(h):
            unit = half * heads + h
            for copy in back_copies(unit):
                copy.wait_recv()
            total = jnp.transpose(
                jnp.broadcast_to(back_total_in[unit], (head, rows))
            )
            mine = own_sum[unit]
            attended[half, :, pl.ds(pl.multiple_of(h * head, head), head)] = (
                (mine[:, 0:head] + back_in[unit].astype(f32))
                / (mine[:, head : 2 * head] + total)
            ).astype(bf16)

    mixed_copy = pltpu.make_async_remote_copy(
        src_ref=mixed_out,
        dst_ref=mixed_in,
        send_sem=mixed_sem.at[0],
        recv_sem=mixed_sem.at[1],
        device_id={"head": other_core},
        device_id_type=MESH,
    )
    full = output_weight.shape[1]
    wide = 512 if full % 512 == 0 else full

    gather_back(1)
    loads[5].wait()

    @pl.loop(0, full // wide)
    def _(c):
        here = pl.ds(pl.multiple_of(c * wide, wide), wide)
        mixed_out[:, here] = jnp.dot(
            attended[1], output_weight[:, here], preferred_element_type=f32
        ).astype(bf16)

    mixed_copy.start()
    gather_back(0)
    mixed_copy.wait_recv()

    @pl.loop(0, full // wide)
    def _(c):
        here = pl.ds(pl.multiple_of(c * wide, wide), wide)
        mixed = jnp.dot(attended[0], output_weight[:, here], preferred_element_type=f32)
        mixed = mixed + mixed_in[:, here].astype(f32)
        updated_ref[:, here] = (
            tokens_ref[:, here].astype(f32) + modulation_ref[2:3, here] * mixed
        ).astype(bf16)

    normed_copy.wait_send()
    mixed_copy.wait_send()

    @pl.loop(0, units)
    def _(i):
        query_copy(i).wait_send()
        for copy in back_copies(i):
            copy.wait_send()

        @pl.when(has_ahead)
        def _():
            forward_copy(i, mate).wait_send()

        @pl.when(has_behind)
        def _():
            for copy in far_copies(i, mate):
                copy.wait_send()


def on_device(
    video_tokens,
    modulation,
    project_weight,
    output_weight,
    norm_gains,
    text_cache,
    text_count,
    video_keep,
    patch_order,
    stale_cache,
):
    head = norm_gains.shape[1]
    rows, model = video_tokens.shape
    width = project_weight.shape[2]
    patch = stale_cache.shape[1]
    text_rows = text_cache.shape[1]
    heads = width // head
    units = 2 * heads
    smem = pl.BlockSpec(memory_space=pltpu.SMEM)
    vmem = pl.BlockSpec(memory_space=pltpu.VMEM)
    hbm = pl.BlockSpec(memory_space=pl.ANY)
    unit_rows = pltpu.VMEM((units, rows, head), bf16)
    unit_totals = pltpu.VMEM((units, 1, rows), f32)
    unit_sums = pltpu.VMEM((units, rows, 2 * head), f32)
    unit_sems = pltpu.SemaphoreType.DMA((2, units))
    return pl.pallas_call(
        kernel,
        out_shape=(
            pltpu.VMEM(video_tokens.shape, bf16),
            pltpu.VMEM(stale_cache.shape, bf16),
        ),
        in_specs=[smem, smem] + [hbm] * 8,
        out_specs=(vmem, vmem),
        scratch_shapes=[
            pltpu.VMEM(video_tokens.shape, bf16),
            pltpu.VMEM(modulation.shape, f32),
            pltpu.VMEM(norm_gains.shape, f32),
            pltpu.VMEM(video_keep.shape, jnp.int32),
            pltpu.VMEM(project_weight.shape, bf16),
            pltpu.VMEM(output_weight.shape, bf16),
            pltpu.VMEM(text_cache.shape, bf16),
            pltpu.VMEM(stale_cache.shape, bf16),
            pltpu.VMEM((2, rows, model), bf16),
            unit_rows,
            unit_rows,
            unit_rows,
            pltpu.VMEM((2, heads, patch, head), bf16),
            pltpu.VMEM((2, heads, patch, 2 * head), bf16),
            pltpu.VMEM((heads, text_rows, head), bf16),
            pltpu.VMEM((heads, text_rows, 2 * head), bf16),
            unit_sums,
            unit_sums,
            unit_rows,
            unit_totals,
            unit_rows,
            unit_totals,
            unit_rows,
            unit_totals,
            unit_rows,
            unit_totals,
            pltpu.VMEM((2, rows, width), bf16),
            pltpu.VMEM((rows, model), bf16),
            pltpu.VMEM((rows, model), bf16),
            pltpu.SemaphoreType.DMA((10,)),
            pltpu.SemaphoreType.DMA((2,)),
            unit_sems,
            unit_sems,
            unit_sems,
            unit_sems,
            unit_sems,
            unit_sems,
            pltpu.SemaphoreType.DMA((2,)),
        ],
        compiler_params=pltpu.CompilerParams(
            collective_id=0, has_side_effects=True, vmem_limit_bytes=60 * 1024 * 1024
        ),
    )(
        patch_order,
        text_count,
        video_tokens,
        modulation,
        norm_gains,
        video_keep,
        project_weight,
        output_weight,
        text_cache,
        stale_cache,
    )


def solution(mesh):
    placed = (
        P(("groups", "section", "head"), None),
        P("groups", None),
        P(None, None, "head"),
        P("head", None),
        P(),
        P(None, "groups", "head"),
        P("groups"),
        P("groups"),
        P("groups"),
        P(None, ("groups", "section"), "head"),
    )
    return jax.shard_map(
        on_device,
        mesh=mesh,
        in_specs=placed,
        out_specs=(P(("groups", "section", "head"), None), P(None, ("groups", "section"), "head")),
        check_vma=False,
    )
```

```python
import jax
import jax.numpy as jnp
from jax import lax
from jax.experimental import pallas as pl
from jax.experimental.pallas import tpu as pltpu
from jax.sharding import PartitionSpec as P

epsilon = 1e-06
log2_e = 1.4426950408889634
MESH = pl.DeviceIdType.MESH
f32 = jnp.float32
bf16 = jnp.bfloat16


def dot_nt(a, b):
    return lax.dot_general(a, b, (((1,), (1,)), ((), ())), preferred_element_type=f32)


def head_norm(rows, gain):
    return rows * lax.rsqrt(jnp.mean(rows * rows, axis=-1, keepdims=True) + epsilon) * gain


def kernel(
    order_ref,
    count_ref,
    tokens_hbm,
    modulation_hbm,
    gains_hbm,
    keep_hbm,
    weight_hbm,
    output_weight_hbm,
    text_hbm,
    stale_hbm,
    updated_ref,
    raw,
    tokens_ref,
    modulation_ref,
    gains_ref,
    keep_ref,
    weight,
    output_weight,
    text,
    stale,
    normed,
    query,
    query_mate,
    query_far,
    keys,
    values,
    text_keys,
    text_values,
    own_sum,
    mate_sum,
    far_out,
    far_total_out,
    far_in,
    far_total_in,
    back_out,
    back_total_out,
    back_in,
    back_total_in,
    attended,
    mixed_out,
    mixed_in,
    partial,
    load_sem,
    normed_sem,
    query_sem,
    forward_sem,
    far_sem,
    far_total_sem,
    back_sem,
    back_total_sem,
    mixed_sem,
):
    count = lax.axis_size("section")
    me = lax.axis_index("section")
    core = lax.axis_index("head")
    other_core = 1 - core
    parity = lax.rem(me, 2)
    mate = me + 1 - 2 * parity
    step = 2 - 4 * parity
    ahead = me + step
    behind = me - step
    has_ahead = jnp.logical_and(ahead >= 0, ahead < count)
    has_behind = jnp.logical_and(behind >= 0, behind < count)
    rows = tokens_hbm.shape[0]
    head = gains_ref.shape[1]
    width = weight.shape[2]
    heads = width // head
    units = 2 * heads
    patch = 2 * rows

    loads = [
        pltpu.make_async_copy(weight_hbm.at[c], weight.at[c], load_sem.at[c]) for c in range(3)
    ]
    loads.append(pltpu.make_async_copy(stale_hbm, stale, load_sem.at[3]))
    loads.append(pltpu.make_async_copy(text_hbm, text, load_sem.at[4]))
    loads.append(pltpu.make_async_copy(output_weight_hbm, output_weight, load_sem.at[5]))
    small = [
        pltpu.make_async_copy(source, target, load_sem.at[6 + place])
        for place, (source, target) in enumerate(
            (
                (tokens_hbm, tokens_ref),
                (modulation_hbm, modulation_ref),
                (gains_hbm, gains_ref),
                (keep_hbm, keep_ref),
            )
        )
    ]
    for load in small:
        load.start()
    loads[0].start()

    barrier = pltpu.get_barrier_semaphore()
    pl.semaphore_signal(barrier, inc=1, device_id={"head": other_core}, device_id_type=MESH)
    pl.semaphore_signal(barrier, inc=1, device_id={"section": mate}, device_id_type=MESH)

    @pl.when(has_ahead)
    def _():
        pl.semaphore_signal(barrier, inc=1, device_id={"section": ahead}, device_id_type=MESH)

    @pl.when(has_behind)
    def _():
        pl.semaphore_signal(barrier, inc=1, device_id={"section": behind}, device_id_type=MESH)

    for load in small:
        load.wait()
    hidden = tokens_ref[...].astype(f32)
    shifted = hidden - jnp.mean(hidden, axis=-1, keepdims=True)
    spread = jnp.mean(shifted * shifted, axis=-1, keepdims=True)
    normed[0] = (
        shifted * lax.rsqrt(spread + epsilon) * (1.0 + modulation_ref[1:2, :])
        + modulation_ref[0:1, :]
    ).astype(bf16)

    pl.semaphore_wait(
        barrier, 2 + has_ahead.astype(jnp.int32) + has_behind.astype(jnp.int32)
    )

    normed_copy = pltpu.make_async_remote_copy(
        src_ref=normed.at[0],
        dst_ref=normed.at[1],
        send_sem=normed_sem.at[0],
        recv_sem=normed_sem.at[1],
        device_id={"head": other_core},
        device_id_type=MESH,
    )
    normed_copy.start()

    def remote(source, target, sems, unit, device):
        return pltpu.make_async_remote_copy(
            src_ref=source.at[unit],
            dst_ref=target.at[unit],
            send_sem=sems.at[0, unit],
            recv_sem=sems.at[1, unit],
            device_id={"section": device},
            device_id_type=MESH,
        )

    def query_copy(unit):
        return remote(query, query_mate, query_sem, unit, mate)

    def forward_copy(unit, device):
        return remote(query_mate, query_far, forward_sem, unit, device)

    def far_copies(unit, device):
        return (
            remote(far_out, far_in, far_sem, unit, device),
            remote(far_total_out, far_total_in, far_total_sem, unit, device),
        )

    def back_copies(unit):
        return (
            remote(back_out, back_in, back_sem, unit, mate),
            remote(back_total_out, back_total_in, back_total_sem, unit, mate),
        )

    factor = head ** (-0.5) * log2_e
    pair = 2 if heads % 2 == 0 else 1
    span = pair * head

    def columns(step_index):
        return pl.ds(pl.multiple_of(step_index * span, span), span)

    def project_queries(half):
        @pl.loop(0, heads // pair)
        def _(c):
            part = jnp.dot(normed[half], weight[0, :, columns(c)], preferred_element_type=f32)
            for j in range(pair):
                unit = half * heads + c * pair + j
                query[unit] = (
                    head_norm(part[:, j * head : (j + 1) * head], gains_ref[0:1, :]) * factor
                ).astype(bf16)
                query_copy(unit).start()

    early = min(3, heads)

    def forward(unit):
        query_copy(unit).wait_recv()

        @pl.when(has_ahead)
        def _():
            forward_copy(unit, ahead).start()

    for load in loads[1:]:
        load.start()
    loads[0].wait()
    project_queries(0)
    normed_copy.wait_recv()
    project_queries(1)
    loads[1].wait()
    loads[2].wait()
    own_rows = pl.ds(pl.multiple_of(core * rows, rows), rows)
    other_rows = pl.ds(pl.multiple_of(other_core * rows, rows), rows)

    @pl.loop(0, heads // pair)
    def _(c):
        for w in range(2):
            part = jnp.dot(
                normed[...].reshape(patch, normed.shape[2]),
                weight[1 + w, :, columns(c)],
                preferred_element_type=f32,
            ).astype(bf16)
            raw[w, own_rows, columns(c)] = part[0:rows]
            raw[w, other_rows, columns(c)] = part[rows:patch]

        @pl.when(c < early)
        def _():
            forward(c)

    @pl.loop(min(early, heads // pair), early)
    def _(i):
        forward(i)

    loads[3].wait()
    loads[4].wait()

    keep_row = keep_ref[pl.ds(pl.multiple_of(me * patch, patch), patch)].astype(f32)
    keep = jnp.transpose(jnp.broadcast_to(keep_row[None, :], (head, patch)))
    text_rows = text.shape[1]
    live = (
        lax.broadcasted_iota(jnp.int32, (text_rows, head), 0) < count_ref[0]
    ).astype(f32)

    @pl.loop(0, heads)
    def _(h):
        lanes = pl.ds(pl.multiple_of(h * head, head), head)
        for version, cache in ((0, raw), (1, stale)):
            keys[version, h] = head_norm(
                cache[0, :, lanes].astype(f32), gains_ref[1:2, :]
            ).astype(bf16)
            values[version, h, :, 0:head] = (cache[1, :, lanes].astype(f32) * keep).astype(bf16)
            values[version, h, :, head : 2 * head] = keep.astype(bf16)
        text_keys[h] = head_norm(text[0, :, lanes].astype(f32), gains_ref[2:3, :]).astype(bf16)
        text_values[h, :, 0:head] = (text[1, :, lanes].astype(f32) * live).astype(bf16)
        text_values[h, :, head : 2 * head] = live.astype(bf16)

    own_slot = order_ref[me]
    mate_version = jnp.where(own_slot < order_ref[mate], 0, 1)
    far_patch = jnp.clip(me - 1 + 2 * parity, 0, count - 1)
    far_version = jnp.where(own_slot < order_ref[far_patch], 0, 1)

    def weighted(queries, key_rows, value_rows):
        weights = jnp.exp2(dot_nt(queries, key_rows)).astype(bf16)
        return jnp.dot(weights, value_rows, preferred_element_type=f32)

    def total_rows(summed):
        return jnp.transpose(summed[:, head : 2 * head])[0:1, :]

    def send_back(unit):
        numerator = mate_sum[unit, :, 0:head]
        totals = total_rows(mate_sum[unit])

        @pl.when(has_ahead)
        def _():
            for copy in far_copies(unit, mate):
                copy.wait_recv()
            back_out[unit] = (numerator + far_in[unit].astype(f32)).astype(bf16)
            back_total_out[unit] = totals + far_total_in[unit]

        @pl.when(jnp.logical_not(has_ahead))
        def _():
            back_out[unit] = numerator.astype(bf16)
            back_total_out[unit] = totals

        for copy in back_copies(unit):
            copy.start()

    ahead_backs = min(2, heads)

    @pl.loop(early, units + 2 * early)
    def _(i):
        @pl.when(i < units)
        def _():
            forward(i)

        unit = i - early

        @pl.when(unit < units)
        def _():
            h = lax.rem(unit, heads)

            @pl.when(has_behind)
            def _():
                forward_copy(unit, mate).wait_recv()
                summed = weighted(query_far[unit], keys[far_version, h], values[far_version, h])
                far_out[unit] = summed[:, 0:head].astype(bf16)
                far_total_out[unit] = total_rows(summed)
                for copy in far_copies(unit, behind):
                    copy.start()

            mate_sum[unit] = weighted(
                query_mate[unit], keys[mate_version, h], values[mate_version, h]
            )
            own_sum[unit] = weighted(query[unit], keys[0, h], values[0, h]) + weighted(
                query[unit], text_keys[h], text_values[h]
            )

        @pl.when(jnp.logical_and(i >= units - ahead_backs, i < units))
        def _():
            send_back(i - units + ahead_backs)

        @pl.when(i >= heads + 2 * early)
        def _():
            send_back(i - 2 * early)

    @pl.loop(ahead_backs, heads)
    def _(i):
        send_back(i)

    def gather_range(half, first, last):
        @pl.loop(first, last)
        def _(h):
            unit = half * heads + h
            for copy in back_copies(unit):
                copy.wait_recv()
            total = jnp.transpose(
                jnp.broadcast_to(back_total_in[unit], (head, rows))
            )
            mine = own_sum[unit]
            attended[half, :, pl.ds(pl.multiple_of(h * head, head), head)] = (
                (mine[:, 0:head] + back_in[unit].astype(f32))
                / (mine[:, head : 2 * head] + total)
            ).astype(bf16)

    mixed_copy = pltpu.make_async_remote_copy(
        src_ref=mixed_out,
        dst_ref=mixed_in,
        send_sem=mixed_sem.at[0],
        recv_sem=mixed_sem.at[1],
        device_id={"head": other_core},
        device_id_type=MESH,
    )
    full = output_weight.shape[1]
    wide = 512 if full % 512 == 0 else full

    gather_range(1, 0, heads)
    loads[5].wait()

    @pl.loop(0, full // wide)
    def _(c):
        here = pl.ds(pl.multiple_of(c * wide, wide), wide)
        mixed_out[:, here] = jnp.dot(
            attended[1], output_weight[:, here], preferred_element_type=f32
        ).astype(bf16)

    mixed_copy.start()
    split = heads - min(2, heads - 1)
    gather_range(0, 0, split)

    @pl.loop(0, full // wide)
    def _(c):
        here = pl.ds(pl.multiple_of(c * wide, wide), wide)
        partial[:, here] = jnp.dot(
            attended[0, :, 0 : split * head],
            output_weight[0 : split * head, here],
            preferred_element_type=f32,
        )

    mixed_copy.wait_recv()

    @pl.loop(0, full // wide)
    def _(c):
        here = pl.ds(pl.multiple_of(c * wide, wide), wide)
        partial[:, here] = partial[:, here] + mixed_in[:, here].astype(f32)

    gather_range(0, split, heads)

    @pl.loop(0, full // wide)
    def _(c):
        here = pl.ds(pl.multiple_of(c * wide, wide), wide)
        mixed = partial[:, here] + jnp.dot(
            attended[0, :, split * head :],
            output_weight[split * head :, here],
            preferred_element_type=f32,
        )
        updated_ref[:, here] = (
            tokens_ref[:, here].astype(f32) + modulation_ref[2:3, here] * mixed
        ).astype(bf16)

    normed_copy.wait_send()
    mixed_copy.wait_send()

    @pl.loop(0, units)
    def _(i):
        query_copy(i).wait_send()
        for copy in back_copies(i):
            copy.wait_send()

        @pl.when(has_ahead)
        def _():
            forward_copy(i, mate).wait_send()

        @pl.when(has_behind)
        def _():
            for copy in far_copies(i, mate):
                copy.wait_send()


def on_device(
    video_tokens,
    modulation,
    project_weight,
    output_weight,
    norm_gains,
    text_cache,
    text_count,
    video_keep,
    patch_order,
    stale_cache,
):
    head = norm_gains.shape[1]
    rows, model = video_tokens.shape
    width = project_weight.shape[2]
    patch = stale_cache.shape[1]
    text_rows = text_cache.shape[1]
    heads = width // head
    units = 2 * heads
    smem = pl.BlockSpec(memory_space=pltpu.SMEM)
    vmem = pl.BlockSpec(memory_space=pltpu.VMEM)
    hbm = pl.BlockSpec(memory_space=pl.ANY)
    unit_rows = pltpu.VMEM((units, rows, head), bf16)
    unit_totals = pltpu.VMEM((units, 1, rows), f32)
    unit_sums = pltpu.VMEM((units, rows, 2 * head), f32)
    unit_sems = pltpu.SemaphoreType.DMA((2, units))
    return pl.pallas_call(
        kernel,
        out_shape=(
            pltpu.VMEM(video_tokens.shape, bf16),
            pltpu.VMEM(stale_cache.shape, bf16),
        ),
        in_specs=[smem, smem] + [hbm] * 8,
        out_specs=(vmem, vmem),
        scratch_shapes=[
            pltpu.VMEM(video_tokens.shape, bf16),
            pltpu.VMEM(modulation.shape, f32),
            pltpu.VMEM(norm_gains.shape, f32),
            pltpu.VMEM(video_keep.shape, jnp.int32),
            pltpu.VMEM(project_weight.shape, bf16),
            pltpu.VMEM(output_weight.shape, bf16),
            pltpu.VMEM(text_cache.shape, bf16),
            pltpu.VMEM(stale_cache.shape, bf16),
            pltpu.VMEM((2, rows, model), bf16),
            unit_rows,
            unit_rows,
            unit_rows,
            pltpu.VMEM((2, heads, patch, head), bf16),
            pltpu.VMEM((2, heads, patch, 2 * head), bf16),
            pltpu.VMEM((heads, text_rows, head), bf16),
            pltpu.VMEM((heads, text_rows, 2 * head), bf16),
            unit_sums,
            unit_sums,
            unit_rows,
            unit_totals,
            unit_rows,
            unit_totals,
            unit_rows,
            unit_totals,
            unit_rows,
            unit_totals,
            pltpu.VMEM((2, rows, width), bf16),
            pltpu.VMEM((rows, model), bf16),
            pltpu.VMEM((rows, model), bf16),
            pltpu.VMEM((rows, model), f32),
            pltpu.SemaphoreType.DMA((10,)),
            pltpu.SemaphoreType.DMA((2,)),
            unit_sems,
            unit_sems,
            unit_sems,
            unit_sems,
            unit_sems,
            unit_sems,
            pltpu.SemaphoreType.DMA((2,)),
        ],
        compiler_params=pltpu.CompilerParams(
            collective_id=0, has_side_effects=True, vmem_limit_bytes=60 * 1024 * 1024
        ),
    )(
        patch_order,
        text_count,
        video_tokens,
        modulation,
        norm_gains,
        video_keep,
        project_weight,
        output_weight,
        text_cache,
        stale_cache,
    )


def solution(mesh):
    placed = (
        P(("groups", "section", "head"), None),
        P("groups", None),
        P(None, None, "head"),
        P("head", None),
        P(),
        P(None, "groups", "head"),
        P("groups"),
        P("groups"),
        P("groups"),
        P(None, ("groups", "section"), "head"),
    )
    return jax.shard_map(
        on_device,
        mesh=mesh,
        in_specs=placed,
        out_specs=(P(("groups", "section", "head"), None), P(None, ("groups", "section"), "head")),
        check_vma=False,
    )
```
